32 devices in a mesh: rep: 4 (over z), exp: 8 (over y, x, core).
Axes of the slice: x: 2, y: 2, z: 4, core: 2. Of those that a mesh axis runs over, the one named last changes fastest.
Arguments:
- tokens: bfloat16 [64, 128, 512], P('rep', 'exp'), may hold values from -48 to 48
- gate: float32 [64, 128], P('rep', 'exp'), may hold values from 0.25 to 1
- route: int32 [4, 8, 256, 1], P('rep', 'exp'), may hold values from 0 to 7; in each aligned block of 256 rows (0 to 255, 256 to 511, ..., all dimensions but the last counted through in order) at most 48 rows name the same one
- cotangent: bfloat16 [64, 128, 512], P('rep', 'exp'), may hold values from -6 to 6
- w_qkv: bfloat16 [512, 1536], replicated, may hold values from -1 to 1
- w_proj: bfloat16 [512, 512], replicated, may hold values from -0.25 to 0.25
- w_up: bfloat16 [8, 2048, 512], P('exp', 'rep'), may hold values from -0.25 to 0.25
- w_down: bfloat16 [8, 2048, 512], P('exp', 'rep'), may hold values from -0.125 to 0.125
Outputs:
- layer_out: bfloat16 [64, 128, 512], P('rep', 'exp')
- input_grad: bfloat16 [64, 128, 512], P('rep', 'exp')
- grad_up: float32 [8, 2048, 512], P('exp', 'rep')
- grad_down: float32 [8, 2048, 512], P('exp', 'rep')
The draws below stay inside these ranges and needn't reach their ends.
Inputs may be any that keep to these rules, and one draw needn't show every extreme that they name: `route`: among the tokens of one tile no expert is named more than 48 times.
All inputs are finite; a program needn't handle non-finite values.
Results may differ from the reference program's by a relative error of at most 0.018.
Values may be sent and summed in bfloat16 or wider, within the bound.
A program may use at most 64 MiB of HBM per device.

```python
import math
import jax
import jax.numpy as jnp
import numpy as np
from jax import lax

D = 512
FF = 2048
HEADS = 16
TROWS = 16
TCOLS = 16
EXPERTS = 8
TOK_DEV = 256
CAP = 48
ROWS = 64
COLS = 128
N_REP = 4
N_EXP = 8


def draw_tokens(key, part):
    key_base = jax.random.fold_in(jax.random.fold_in(key, 11), 0)
    base = jax.random.normal(key_base, (ROWS, COLS, D), jnp.float32)
    return jnp.clip(base, -48.0, 48.0).astype(jnp.bfloat16)


def draw_w_qkv(key, part):
    key_main = jax.random.fold_in(jax.random.fold_in(key, 23), 0)
    matrix = jnp.clip(jax.random.normal(key_main, (D, 3 * D), jnp.float32), -6.0, 6.0) / jnp.sqrt(jnp.float32(D))
    return matrix.astype(jnp.bfloat16)


def steps_of(key, extent, cuts, smallest, high):
    loudness, own = 1.0, jax.random.fold_in(key, 6)
    for dim, shards_of in cuts:
        draws = jnp.exp(jax.random.uniform(jax.random.fold_in(own, dim), (shards_of,), jnp.float32, smallest / len(cuts), high / len(cuts)))
        loudness = loudness * jnp.repeat(draws, extent[dim] // shards_of).reshape([-1 if axis == dim else 1 for axis in range(len(extent))])
    return loudness


def assign_block(own_key, own, number, rows, amount, top, limit, slope):
    ranking = jax.random.permutation(own_key, amount)
    packed, common = shares(amount, rows * top, limit, slope, True), shares(amount, rows * top, limit, slope, False)
    places = jnp.arange(amount)

    def named(sizes, offset_by):
        used = int((sizes > 0).sum())
        fixed = max(1, used // 4)
        shifted = fixed + (places - fixed + offset_by * (used - fixed)) % max(1, amount - fixed)
        return jnp.zeros((amount,), jnp.int32).at[ranking[jnp.where(places < fixed, places, shifted)]].set(jnp.asarray(sizes, jnp.int32))

    sizes = jnp.where(number % 4 == 0, named(packed, number // 4), named(common, number - number // 4 - 1))
    mixed = jax.random.permutation(jax.random.fold_in(own, 3), amount)
    source_of, receiver = mixed[0:amount // 2 * 2:2], mixed[1:amount // 2 * 2:2]
    margin = jnp.minimum(sizes[source_of] - 1, limit - sizes[receiver]) // 2
    margin = jnp.where((source_of == ranking[0]) | (receiver == ranking[0]) | (sizes[receiver] == 0), 0, jnp.maximum(margin, 0))
    shifted = jax.random.randint(jax.random.fold_in(own, 4), (amount // 2,), 0, 1 << 20) % (margin + 1)
    sizes = sizes.at[source_of].add(-shifted).at[receiver].add(shifted)
    members = jnp.searchsorted(jnp.cumsum(sizes), jnp.arange(rows * top), side="right").astype(jnp.int32)
    listing = members.reshape(top, rows).T
    listing = listing[jax.random.permutation(jax.random.fold_in(own, 1), rows)]
    offset_by = jax.random.randint(jax.random.fold_in(own, 2), (rows, 1), 0, top)
    return jnp.take_along_axis(listing, (jnp.arange(top)[None, :] + offset_by) % top, axis=1)


def shares(amount, total, most, lean, full):
    loads = [(1 << 20) // math.isqrt(rank ** lean) + 1 for rank in range(1, amount + 1)]
    largest = most if full else min(most, max(-(-total // amount), total * loads[0] // sum(loads)))
    least = 1 if total - largest >= amount - 1 else 0
    holding, rest = [largest] + [least] * (amount - 1), total - largest - least * (amount - 1)
    while rest > 0:
        movable = [i for i in range(1, amount) if holding[i] < largest] or [i for i in range(1, amount) if holding[i] < most]
        pool, remaining = sum([loads[i] for i in movable]), rest
        for i in movable:
            addition = min(most - holding[i], max(1, remaining * loads[i] // pool), rest)
            holding[i] = holding[i] + addition
            rest = rest - addition
    return np.array(holding)


def normal_values(own_key, shape, width, most, cuts=(), kind=jnp.bfloat16):
    gain = steps_of(own_key, shape, cuts, -0.22, 0.18) if cuts else 1.0
    result = jax.random.normal(own_key, shape, jnp.float32) * width * gain
    return jnp.minimum(jnp.maximum(result, -most), most).astype(kind)


def setup_inputs(seed: int = 0) -> dict:
    splits = jax.random.split(jax.random.key(seed), 9)
    tokens = draw_tokens(jax.random.fold_in(splits[8], 71), 0)
    gate = jnp.clip(0.25 + 0.75 * jax.random.uniform(splits[1], (ROWS, COLS), jnp.float32) ** steps_of(splits[1], (ROWS, COLS), ((0, 4), (1, 8)), -0.2, 0.2), 0.25, 1.0)
    route_keys = jax.random.split(jax.random.fold_in(splits[2], 1), N_REP * N_EXP * TOK_DEV // TOK_DEV)
    route_turns = jax.random.permutation(jax.random.fold_in(splits[2], 3), N_REP * N_EXP * TOK_DEV // TOK_DEV)
    route = jax.vmap(lambda own, number: assign_block(jax.random.fold_in(splits[2], 2), own, number, TOK_DEV, EXPERTS, 1, CAP, 2))(route_keys, route_turns).reshape((N_REP, N_EXP, TOK_DEV, 1))
    cotangent = normal_values(splits[3], (ROWS, COLS, D), 1.0, 6.0, ((0, 4), (1, 8)))
    w_qkv = draw_w_qkv(jax.random.fold_in(splits[8], 71), 0)
    w_proj = normal_values(splits[5], (D, D), D ** -0.5, 0.25)
    w_up = normal_values(splits[6], (EXPERTS, FF, D), D ** -0.5, 0.25, ((0, 8), (1, 4)))
    w_down = normal_values(splits[7], (EXPERTS, FF, D), FF ** -0.5, 0.125, ((0, 8), (1, 4)))
    return {"tokens": tokens, "gate": gate, "route": route, "cotangent": cotangent, "w_qkv": w_qkv, "w_proj": w_proj, "w_up": w_up, "w_down": w_down}


GELU_C = math.sqrt(2.0 / math.pi)
window_side = 8
margin_cells = 4

def gelu_tanh(inputs):
    return 0.5 * inputs * (1.0 + jnp.tanh(GELU_C * (inputs + 0.044715 * inputs * inputs * inputs)))

def gelu_slope(inputs):
    inner = jnp.tanh(GELU_C * (inputs + 0.044715 * inputs * inputs * inputs))
    return 0.5 * (1.0 + inner) + 0.5 * inputs * (1.0 - inner * inner) * GELU_C * (1.0 + 3.0 * 0.044715 * inputs * inputs)

def layer_norm(values):
    average = lax.optimization_barrier(jnp.mean(values, axis=-1, keepdims=True))
    centred = values - average
    spread = lax.optimization_barrier(jnp.mean(centred * centred, axis=-1, keepdims=True))
    return centred * lax.rsqrt(spread + 1e-05)

def window_attend(qkv, in_grid):
    ext_rows, ext_cols, triple = qkv.shape
    feature = triple // 3
    head_size = feature // HEADS
    win_rows = ext_rows // window_side
    win_cols = ext_cols // window_side
    cells = window_side * window_side
    blocks = qkv.reshape(win_rows, window_side, win_cols, window_side, triple).transpose(0, 2, 1, 3, 4)
    blocks = blocks.reshape(win_rows * win_cols, cells, 3, HEADS, head_size)
    present = in_grid.reshape(win_rows, window_side, win_cols, window_side).transpose(0, 2, 1, 3).reshape(win_rows * win_cols, cells)
    queries = blocks[:, :, 0].astype(jnp.float32)
    key_part = blocks[:, :, 1].astype(jnp.float32)
    value_part = blocks[:, :, 2].astype(jnp.float32)
    scores = jnp.einsum('wqhd,wkhd->whqk', queries, key_part) / math.sqrt(head_size)
    scores = jnp.where(present[:, None, None, :], scores, jnp.float32(-1e+30))
    peak_score = lax.optimization_barrier(jnp.max(scores, axis=-1, keepdims=True))
    weights = jnp.exp(scores - peak_score)
    probabilities = (weights / lax.optimization_barrier(jnp.sum(weights, axis=-1, keepdims=True))).astype(jnp.bfloat16)
    context = jnp.einsum('whqk,wkhd->wqhd', probabilities.astype(jnp.float32), value_part).astype(jnp.bfloat16)
    context = context.reshape(win_rows, win_cols, window_side, window_side, feature).transpose(0, 2, 1, 3, 4)
    return context.reshape(ext_rows, ext_cols, feature)

def to_devices(values):
    return values.reshape(N_REP, TROWS, N_EXP, TCOLS, -1).transpose(0, 2, 1, 3, 4).reshape(N_REP, N_EXP, TOK_DEV, -1)

def to_grid(values):
    return values.reshape(N_REP, N_EXP, TROWS, TCOLS, -1).transpose(0, 2, 1, 3, 4).reshape(N_REP * TROWS, N_EXP * TCOLS, -1)

def one_replica(slot_rows, slot_grads, up_mat, down_mat):
    pre_act = jnp.dot(slot_rows, up_mat.T, preferred_element_type=jnp.float32)
    hidden = gelu_tanh(pre_act).astype(jnp.bfloat16)
    expert_out = jnp.dot(hidden, down_mat, preferred_element_type=jnp.float32).astype(jnp.bfloat16)
    hidden_grad = jnp.dot(slot_grads, down_mat.T, preferred_element_type=jnp.float32)
    pre_grad = (hidden_grad * gelu_slope(pre_act)).astype(jnp.bfloat16)
    input_slots = jnp.dot(pre_grad, up_mat, preferred_element_type=jnp.float32).astype(jnp.bfloat16)
    part_up = jnp.dot(pre_grad.T, slot_rows, preferred_element_type=jnp.float32).astype(jnp.bfloat16)
    part_down = jnp.dot(hidden.T, slot_grads, preferred_element_type=jnp.float32).astype(jnp.bfloat16)
    return (expert_out, input_slots, part_up, part_down)

def one_expert(operands):
    rows_all, grads_all, up_mat, down_mat = operands
    expert_out, input_slots, part_up, part_down = jax.vmap(one_replica, in_axes=(0, 0, None, None))(rows_all, grads_all, up_mat, down_mat)
    grad_up = lax.optimization_barrier(jnp.sum(part_up.astype(jnp.float32), axis=0)) / N_REP
    grad_down = lax.optimization_barrier(jnp.sum(part_down.astype(jnp.float32), axis=0)) / N_REP
    return (expert_out, input_slots, grad_up, grad_down)

def reference(tokens, gate, route, cotangent, w_qkv, w_proj, w_up, w_down):
    grid_rows, grid_cols, feature = tokens.shape
    padded = jnp.pad(tokens, ((margin_cells, margin_cells), (margin_cells, margin_cells), (0, 0)))
    ext_rows = grid_rows + 2 * margin_cells
    ext_cols = grid_cols + 2 * margin_cells
    qkv_all = jnp.dot(padded.reshape(-1, feature), w_qkv, preferred_element_type=jnp.float32).astype(jnp.bfloat16)
    qkv_all = qkv_all.reshape(ext_rows, ext_cols, 3 * feature)
    row_ids = jnp.arange(ext_rows, dtype=jnp.int32) - margin_cells
    col_ids = jnp.arange(ext_cols, dtype=jnp.int32) - margin_cells
    in_grid = ((row_ids >= 0) & (row_ids < grid_rows))[:, None] & ((col_ids >= 0) & (col_ids < grid_cols))[None, :]
    context = window_attend(qkv_all, in_grid)[margin_cells:grid_rows + margin_cells, margin_cells:grid_cols + margin_cells].reshape(-1, feature)
    attended = jnp.dot(context, w_proj, preferred_element_type=jnp.float32)
    mixed = (tokens.reshape(-1, feature).astype(jnp.float32) + layer_norm(attended)).astype(jnp.bfloat16)
    mixed_dev = to_devices(mixed.reshape(grid_rows, grid_cols, feature))
    gate_dev = to_devices(gate[:, :, None])[..., 0]
    upstream = (gate[:, :, None] * cotangent.astype(jnp.float32)).astype(jnp.bfloat16)
    upstream_dev = to_devices(upstream)
    chosen = route[..., 0]
    matches = (chosen[..., None] == jnp.arange(EXPERTS, dtype=jnp.int32)).astype(jnp.int32)
    position = lax.optimization_barrier(jnp.sum(matches * (jnp.cumsum(matches, axis=2) - 1), axis=-1)).astype(jnp.int32)
    replica = jnp.arange(N_REP, dtype=jnp.int32)[:, None, None]
    source = jnp.arange(N_EXP, dtype=jnp.int32)[None, :, None]
    target = (((replica * EXPERTS + chosen) * N_EXP + source) * CAP + position).reshape(-1).astype(jnp.int32)
    total = N_REP * EXPERTS * N_EXP * CAP
    slots_x = jnp.zeros((total, feature), jnp.bfloat16).at[target].set(mixed_dev.reshape(-1, feature))
    slots_g = jnp.zeros((total, feature), jnp.bfloat16).at[target].set(upstream_dev.reshape(-1, feature))
    slots_x = slots_x.reshape(N_REP, EXPERTS, N_EXP * CAP, feature).transpose(1, 0, 2, 3)
    slots_g = slots_g.reshape(N_REP, EXPERTS, N_EXP * CAP, feature).transpose(1, 0, 2, 3)
    expert_out, input_slots, grad_up, grad_down = lax.map(one_expert, (slots_x, slots_g, w_up, w_down))
    out_flat = expert_out.transpose(1, 0, 2, 3).reshape(total, feature)
    back_flat = input_slots.transpose(1, 0, 2, 3).reshape(total, feature)
    out_tok = out_flat[target].reshape(N_REP, N_EXP, TOK_DEV, feature).astype(jnp.float32)
    grad_tok = back_flat[target].reshape(N_REP, N_EXP, TOK_DEV, feature)
    layer_dev = (mixed_dev.astype(jnp.float32) + gate_dev[..., None] * out_tok).astype(jnp.bfloat16)
    return (to_grid(layer_dev), to_grid(grad_tok), grad_up, grad_down)
```

```python
import math

import jax
import jax.numpy as jnp
from jax import lax
from jax.experimental import pallas as pl
from jax.experimental.pallas import tpu as pltpu
from jax.sharding import PartitionSpec as P

HEADS = 16


GELU_C = math.sqrt(2.0 / math.pi)
window_side = 8
margin_cells = 4


def padded(block, sides, width):
    for axis, dim in sides:
        count = lax.axis_size(axis)
        forward = [(i, i + 1) for i in range(count - 1)]
        backward = [(target, source) for source, target in forward]
        low = lax.ppermute(
            lax.slice_in_dim(block, block.shape[dim] - width, None, axis=dim), axis, forward
        )
        high = lax.ppermute(lax.slice_in_dim(block, 0, width, axis=dim), axis, backward)
        block = jnp.concatenate([low, block, high], axis=dim)
    return block


def gelu_tanh(inputs):
    return 0.5 * inputs * (1.0 + jnp.tanh(GELU_C * (inputs + 0.044715 * inputs * inputs * inputs)))


def gelu_slope(inputs):
    inner = jnp.tanh(GELU_C * (inputs + 0.044715 * inputs * inputs * inputs))
    return 0.5 * (1.0 + inner) + 0.5 * inputs * (1.0 - inner * inner) * GELU_C * (
        1.0 + 3.0 * 0.044715 * inputs * inputs
    )


def layer_norm(values):
    average = jnp.mean(values, axis=-1, keepdims=True)
    centred = values - average
    spread = jnp.mean(centred * centred, axis=-1, keepdims=True)
    return centred * lax.rsqrt(spread + 1e-05)


def window_attend(qkv, in_grid):
    ext_rows, ext_cols, triple = qkv.shape
    feature = triple // 3
    head_size = feature // HEADS
    win_rows = ext_rows // window_side
    win_cols = ext_cols // window_side
    cells = window_side * window_side
    blocks = qkv.reshape(win_rows, window_side, win_cols, window_side, triple).transpose(
        0, 2, 1, 3, 4
    )
    blocks = blocks.reshape(win_rows * win_cols, cells, 3, HEADS, head_size)
    present = (
        in_grid.reshape(win_rows, window_side, win_cols, window_side)
        .transpose(0, 2, 1, 3)
        .reshape(win_rows * win_cols, cells)
    )
    scores = jnp.einsum(
        "wqhd,wkhd->whqk", blocks[:, :, 0], blocks[:, :, 1], preferred_element_type=jnp.float32
    ) / math.sqrt(head_size)
    scores = jnp.where(present[:, None, None, :], scores, jnp.float32(-1e30))
    peak_score = jnp.max(scores, axis=-1, keepdims=True)
    weights = jnp.exp(scores - peak_score)
    probabilities = (weights / jnp.sum(weights, axis=-1, keepdims=True)).astype(jnp.bfloat16)
    context = jnp.einsum(
        "whqk,wkhd->wqhd", probabilities, blocks[:, :, 2], preferred_element_type=jnp.float32
    ).astype(jnp.bfloat16)
    context = context.reshape(win_rows, win_cols, window_side, window_side, feature).transpose(
        0, 2, 1, 3, 4
    )
    return context.reshape(ext_rows, ext_cols, feature)


def enter(ring, ranks):
    barrier = pltpu.get_barrier_semaphore()
    me, row = lax.axis_index("exp"), lax.axis_index("rep")

    def greet(step, carry):
        pl.semaphore_signal(barrier, device_id={"exp": lax.rem(me + step, ring)})
        return carry

    lax.fori_loop(1, ring, greet, 0)

    @pl.when(row > 0)
    def _():
        pl.semaphore_signal(barrier, device_id={"rep": row - 1})

    @pl.when(row < ranks - 1)
    def _():
        pl.semaphore_signal(barrier, device_id={"rep": row + 1})

    below = (row + ranks - 1) // ranks
    above = (2 * ranks - 2 - row) // ranks
    pl.semaphore_wait(barrier, ring - 1 + below + above)


def swap_start(ring, cap, source, target, send_sem, recv_sem):
    me = lax.axis_index("exp")
    mine = pl.ds(pl.multiple_of(me * cap, 16), cap)

    def send(step, carry):
        peer = lax.rem(me + step, ring)
        pltpu.make_async_remote_copy(
            src_ref=source.at[pl.ds(pl.multiple_of(peer * cap, 16), cap)],
            dst_ref=target.at[mine],
            send_sem=send_sem,
            recv_sem=recv_sem,
            device_id={"exp": peer},
        ).start()
        return carry

    lax.fori_loop(1, ring, send, 0)
    pltpu.make_async_copy(source.at[mine], target.at[mine], recv_sem).start()


def await_bytes(ref, sem):
    pltpu.make_async_copy(ref, ref, sem).wait()


def spread_kernel(
    count, ring, ranks, cap, values, placers, out, held, slots, z_send, z_recv, a_send, a_recv
):
    row = lax.axis_index("rep")
    enter(ring, ranks)

    def pass_on(t, origin, source, side):
        pltpu.make_async_remote_copy(
            src_ref=source,
            dst_ref=held.at[t, origin],
            send_sem=z_send.at[t, origin, (side + 1) // 2],
            recv_sem=z_recv.at[t, origin],
            device_id={"rep": row + side},
        ).start()

    def dispatch(t, origin, tokens):
        slots[t, origin] = jnp.dot(
            placers[origin], tokens, preferred_element_type=jnp.float32
        ).astype(jnp.bfloat16)
        swap_start(
            ring, cap, slots.at[t, origin], out.at[t, origin], a_send.at[t, origin], a_recv.at[t, origin]
        )

    for t in range(count):

        @pl.when(row < ranks - 1)
        def _():
            pass_on(t, row, values[t], 1)

        @pl.when(row > 0)
        def _():
            pass_on(t, row, values[t], -1)

    for t in range(count):
        dispatch(t, row, values[t][...])

    def step(k, carry):
        for t in range(count):
            for side in (1, -1):
                origin = row - side * k

                @pl.when((origin >= 0) & (origin < ranks))
                def _():
                    await_bytes(held.at[t, origin], z_recv.at[t, origin])
                    onward = row + side

                    @pl.when((onward >= 0) & (onward < ranks))
                    def _():
                        pass_on(t, origin, held.at[t, origin], side)

                    dispatch(t, origin, held[t, origin])

        return carry

    lax.fori_loop(1, ranks, step, 0)

    def finish(origin, carry):
        for t in range(count):
            await_bytes(out.at[t, origin], a_recv.at[t, origin])
            sent = slots.at[t, origin, pl.ds(0, (ring - 1) * cap)]
            await_bytes(sent, a_send.at[t, origin])

            @pl.when((origin <= row) & (row < ranks - 1))
            def _():
                await_bytes(held.at[t, origin], z_send.at[t, origin, 1])

            @pl.when((origin >= row) & (row > 0))
            def _():
                await_bytes(held.at[t, origin], z_send.at[t, origin, 0])

        return carry

    lax.fori_loop(0, ranks, finish, 0)


def collect_kernel(
    count, ring, ranks, cap, parts, placers, out, back, sums, z_send, z_recv, a_send, a_recv
):
    row = lax.axis_index("rep")
    enter(ring, ranks)

    def launch(t, target):
        swap_start(
            ring, cap, parts[t].at[target], back.at[t, target], a_send.at[t, target], a_recv.at[t, target]
        )

    def ahead(step, carry):
        k = ranks - step
        for t in range(count):
            for side in (1, -1):
                target = row + side * k

                @pl.when((target >= 0) & (target < ranks))
                def _():
                    launch(t, target)

        return carry

    lax.fori_loop(1, ranks, ahead, 0)
    for t in range(count):
        launch(t, row)

    def placed(t, target):
        await_bytes(back.at[t, target], a_recv.at[t, target])
        return jnp.dot(placers[target], back[t, target], preferred_element_type=jnp.float32)

    def step(index, carry):
        k = ranks - index
        for t in range(count):
            for side in (1, -1):
                target = row + side * k

                @pl.when((target >= 0) & (target < ranks))
                def _():
                    own = placed(t, target)
                    behind = row - side
                    first = (behind < 0) | (behind >= ranks)

                    @pl.when(first)
                    def _():
                        sums[t, target] = own.astype(jnp.bfloat16)

                    @pl.when(jnp.logical_not(first))
                    def _():
                        await_bytes(sums.at[t, target], z_recv.at[t, target])
                        total = own + sums[t, target].astype(jnp.float32)
                        sums[t, target] = total.astype(jnp.bfloat16)

                    final = ranks if side < 0 else target
                    place = jnp.where(k == 1, final, target)
                    pltpu.make_async_remote_copy(
                        src_ref=sums.at[t, target],
                        dst_ref=sums.at[t, place],
                        send_sem=z_send.at[t, target],
                        recv_sem=z_recv.at[t, place],
                        device_id={"rep": row + side},
                    ).start()

        return carry

    lax.fori_loop(1, ranks, step, 0)
    for t in range(count):
        out[t] = placed(t, row)

        @pl.when(row > 0)
        def _():
            await_bytes(sums.at[t, row], z_recv.at[t, row])
            out[t] += sums[t, row].astype(jnp.float32)

        @pl.when(row < ranks - 1)
        def _():
            await_bytes(sums.at[t, ranks], z_recv.at[t, ranks])
            out[t] += sums[t, ranks].astype(jnp.float32)

    def finish(target, carry):
        for t in range(count):
            sent = back.at[t, target, pl.ds(0, (ring - 1) * cap)]
            await_bytes(sent, a_send.at[t, target])

            @pl.when(target != row)
            def _():
                await_bytes(sums.at[t, target], z_send.at[t, target])

        return carry

    lax.fori_loop(0, ranks, finish, 0)


def in_vmem(amount):
    return [pl.BlockSpec(memory_space=pltpu.VMEM)] * amount


def spread(values, placers, ring, ranks, cap):
    count = len(values)
    tok, feature = values[0].shape

    def body(*refs):
        spread_kernel(count, ring, ranks, cap, refs[:count], *refs[count:])

    rows = ring * cap
    return pl.pallas_call(
        body,
        name="spread",
        out_shape=jax.ShapeDtypeStruct((count, ranks, rows, feature), jnp.bfloat16),
        in_specs=in_vmem(count + 1),
        out_specs=pl.BlockSpec(memory_space=pltpu.VMEM),
        scratch_shapes=[
            pltpu.VMEM((count, ranks, tok, feature), jnp.bfloat16),
            pltpu.VMEM((count, ranks, rows, feature), jnp.bfloat16),
            pltpu.SemaphoreType.DMA((count, ranks, 2)),
            pltpu.SemaphoreType.DMA((count, ranks)),
            pltpu.SemaphoreType.DMA((count, ranks)),
            pltpu.SemaphoreType.DMA((count, ranks)),
        ],
        compiler_params=pltpu.CompilerParams(
            collective_id=0, has_side_effects=True, vmem_limit_bytes=60 << 20
        ),
    )(*values, placers)


def collect(parts, placers, ring, ranks, cap):
    count = len(parts)
    rows, feature = parts[0].shape[1:]
    tok = placers.shape[1]

    def body(*refs):
        collect_kernel(count, ring, ranks, cap, refs[:count], *refs[count:])

    return pl.pallas_call(
        body,
        name="collect",
        out_shape=jax.ShapeDtypeStruct((count, tok, feature), jnp.float32),
        in_specs=in_vmem(count + 1),
        out_specs=pl.BlockSpec(memory_space=pltpu.VMEM),
        scratch_shapes=[
            pltpu.VMEM((count, ranks, rows, feature), jnp.bfloat16),
            pltpu.VMEM((count, ranks + 1, tok, feature), jnp.bfloat16),
            pltpu.SemaphoreType.DMA((count, ranks)),
            pltpu.SemaphoreType.DMA((count, ranks + 1)),
            pltpu.SemaphoreType.DMA((count, ranks)),
            pltpu.SemaphoreType.DMA((count, ranks)),
        ],
        compiler_params=pltpu.CompilerParams(
            collective_id=1, has_side_effects=True, vmem_limit_bytes=60 << 20
        ),
    )(*parts, placers)


def per_device(tokens, gate, route, cotangent, w_qkv, w_proj, w_up, w_down):
    tile_rows, tile_cols, feature = tokens.shape
    tok_count = tile_rows * tile_cols
    ext_rows = tile_rows + 2 * margin_cells
    ext_cols = tile_cols + 2 * margin_cells
    extended = padded(tokens, (("rep", 0), ("exp", 1)), 4)
    qkv = jnp.dot(extended.reshape(-1, feature), w_qkv, preferred_element_type=jnp.float32).astype(
        jnp.bfloat16
    )
    qkv = qkv.reshape(ext_rows, ext_cols, 3 * feature)
    row_ids = (
        lax.axis_index("rep") * tile_rows - margin_cells + jnp.arange(ext_rows, dtype=jnp.int32)
    )
    col_ids = (
        lax.axis_index("exp") * tile_cols - margin_cells + jnp.arange(ext_cols, dtype=jnp.int32)
    )
    row_inside = (row_ids >= 0) & (row_ids < tile_rows * lax.axis_size("rep"))
    col_inside = (col_ids >= 0) & (col_ids < tile_cols * lax.axis_size("exp"))
    in_grid = row_inside[:, None] & col_inside[None, :]
    context = window_attend(qkv, in_grid)[
        margin_cells : tile_rows + margin_cells, margin_cells : tile_cols + margin_cells
    ].reshape(tok_count, feature)
    attended = jnp.dot(context, w_proj, preferred_element_type=jnp.float32)
    flat_tokens = tokens.reshape(tok_count, feature)
    mixed = (flat_tokens.astype(jnp.float32) + layer_norm(attended)).astype(jnp.bfloat16)
    experts = lax.axis_size("exp")
    ranks = lax.axis_size("rep")
    capacity = max(2, 3 * tok_count // (2 * experts))
    capacity = -(-capacity // 16) * 16
    slot_count = experts * capacity
    chosen = route.reshape(tok_count)
    matches = (chosen[:, None] == jnp.arange(experts, dtype=jnp.int32)[None, :]).astype(jnp.int32)
    position = jnp.sum(matches * (jnp.cumsum(matches, axis=0) - 1), axis=1)
    targets = lax.all_gather(chosen * capacity + position, "rep")
    slot_ids = jnp.arange(slot_count, dtype=jnp.int32)
    to_slots = (slot_ids[None, :, None] == targets[:, None, :]).astype(jnp.bfloat16)
    from_slots = (targets[:, :, None] == slot_ids[None, None, :]).astype(jnp.bfloat16)
    gate_rows = gate.reshape(tok_count)
    upstream = (
        gate_rows[:, None] * cotangent.reshape(tok_count, feature).astype(jnp.float32)
    ).astype(jnp.bfloat16)
    gathered = spread((upstream, mixed), to_slots, experts, ranks, capacity)
    slot_grads = gathered[0].reshape(-1, feature)
    slot_rows = gathered[1].reshape(-1, feature)
    up_mat = w_up[0]
    down_mat = w_down[0]
    pre_act = lax.dot_general(
        slot_rows, up_mat, (((1,), (1,)), ((), ())), preferred_element_type=jnp.float32
    )
    hidden = gelu_tanh(pre_act).astype(jnp.bfloat16)
    expert_out = jnp.dot(hidden, down_mat, preferred_element_type=jnp.float32).astype(jnp.bfloat16)
    hidden_grad = lax.dot_general(
        slot_grads, down_mat, (((1,), (1,)), ((), ())), preferred_element_type=jnp.float32
    )
    pre_grad = (hidden_grad * gelu_slope(pre_act)).astype(jnp.bfloat16)
    input_slots = jnp.dot(pre_grad, up_mat, preferred_element_type=jnp.float32).astype(jnp.bfloat16)
    shape = (ranks, slot_count, feature)
    returned = collect(
        (expert_out.reshape(shape), input_slots.reshape(shape)), from_slots, experts, ranks, capacity
    )
    layer_out = (mixed.astype(jnp.float32) + gate_rows[:, None] * returned[0]).astype(jnp.bfloat16)
    input_grad = returned[1].astype(jnp.bfloat16)
    average_factor = 1.0 / ranks
    grad_up = lax.dot_general(
        pre_grad, slot_rows, (((0,), (0,)), ((), ())), preferred_element_type=jnp.float32
    )
    grad_down = lax.dot_general(
        hidden, slot_grads, (((0,), (0,)), ((), ())), preferred_element_type=jnp.float32
    )
    return (
        layer_out.reshape(tile_rows, tile_cols, feature),
        input_grad.reshape(tile_rows, tile_cols, feature),
        (grad_up * average_factor)[None],
        (grad_down * average_factor)[None],
    )


def solution(mesh):
    placed = (
        P("rep", "exp", None),
        P("rep", "exp"),
        P("rep", "exp", None, None),
        P("rep", "exp", None),
        P(),
        P(),
        P("exp", "rep", None),
        P("exp", "rep", None),
    )
    return jax.shard_map(
        per_device,
        mesh=mesh,
        in_specs=placed,
        out_specs=(
            P("rep", "exp", None),
            P("rep", "exp", None),
            P("exp", "rep", None),
            P("exp", "rep", None),
        ),
        check_vma=False,
    )
```

```python
import math

import jax
import jax.numpy as jnp
import numpy as np
from jax import lax
from jax.experimental import pallas as pl
from jax.experimental.pallas import tpu as pltpu
from jax.sharding import PartitionSpec as P

HEADS = 16


GELU_C = math.sqrt(2.0 / math.pi)
window_side = 8
margin_cells = 4


def padded(block, sides, width):
    for axis, dim in sides:
        count = lax.axis_size(axis)
        forward = [(i, i + 1) for i in range(count - 1)]
        backward = [(target, source) for source, target in forward]
        low = lax.ppermute(
            lax.slice_in_dim(block, block.shape[dim] - width, None, axis=dim), axis, forward
        )
        high = lax.ppermute(lax.slice_in_dim(block, 0, width, axis=dim), axis, backward)
        block = jnp.concatenate([low, block, high], axis=dim)
    return block


def gelu_tanh(inputs):
    return 0.5 * inputs * (1.0 + jnp.tanh(GELU_C * (inputs + 0.044715 * inputs * inputs * inputs)))


def gelu_slope(inputs):
    inner = jnp.tanh(GELU_C * (inputs + 0.044715 * inputs * inputs * inputs))
    return 0.5 * (1.0 + inner) + 0.5 * inputs * (1.0 - inner * inner) * GELU_C * (
        1.0 + 3.0 * 0.044715 * inputs * inputs
    )


def layer_norm(values):
    average = jnp.mean(values, axis=-1, keepdims=True)
    centred = values - average
    spread = jnp.mean(centred * centred, axis=-1, keepdims=True)
    return centred * lax.rsqrt(spread + 1e-05)


def window_order(tile_rows, tile_cols):
    wins = (tile_cols + 2 * margin_cells) // window_side
    rows = (np.arange(tile_rows) + margin_cells) // window_side
    cols = (np.arange(tile_cols) + margin_cells) // window_side
    window = (rows[:, None] * wins + cols[None, :]).reshape(-1)
    order = np.argsort(window, kind="stable")
    counts = np.bincount(window)
    return order, tuple((int(c.sum()), int(n)) for c, n in ((counts[:i], counts[i]) for i in range(len(counts))))


def attend_window(number, first, amount, queries, keys_values, absent, context):
    feature = queries.shape[1]
    head_size = feature // HEADS
    cells = window_side * window_side
    group = 128 // head_size
    mine = pl.ds(first, amount)
    theirs = pl.ds(number * cells, cells)
    lane = lax.broadcasted_iota(jnp.int32, (amount, 128), 1)
    keep = [
        ((lane >= h * head_size) & (lane < (h + 1) * head_size)).astype(jnp.float32)
        for h in range(group)
    ]
    for start in range(0, feature, 128):
        query = queries[mine, pl.ds(start, 128)]
        stacked = jnp.concatenate([query * k.astype(jnp.bfloat16) for k in keep], axis=0)
        scores = lax.dot_general(
            stacked,
            keys_values[theirs, pl.ds(start, 128)],
            (((1,), (1,)), ((), ())),
            preferred_element_type=jnp.float32,
        ) / math.sqrt(head_size)
        scores = scores + absent[pl.ds(number, 1), :]
        weights = jnp.exp(scores - jnp.max(scores, axis=-1, keepdims=True))
        total = jnp.sum(weights, axis=-1, keepdims=True)
        probabilities = (weights * (1.0 / total)).astype(jnp.bfloat16)
        mixed = jnp.dot(
            probabilities,
            keys_values[theirs, pl.ds(feature + start, 128)],
            preferred_element_type=jnp.float32,
        )
        picked = sum(k * mixed[h * amount : (h + 1) * amount] for h, k in enumerate(keep))
        context[mine, pl.ds(start, 128)] = picked.astype(jnp.bfloat16)


def enter(ring, ranks):
    barrier = pltpu.get_barrier_semaphore()
    me, row = lax.axis_index("exp"), lax.axis_index("rep")

    def greet(step, carry):
        pl.semaphore_signal(barrier, device_id={"exp": lax.rem(me + step, ring)})
        return carry

    lax.fori_loop(1, ring, greet, 0)

    @pl.when(row > 0)
    def _():
        pl.semaphore_signal(barrier, device_id={"rep": row - 1})

    @pl.when(row < ranks - 1)
    def _():
        pl.semaphore_signal(barrier, device_id={"rep": row + 1})

    below = (row + ranks - 1) // ranks
    above = (2 * ranks - 2 - row) // ranks
    pl.semaphore_wait(barrier, ring - 1 + below + above)


def swap_start(ring, cap, source, target, send_sem, recv_sem):
    me = lax.axis_index("exp")
    mine = pl.ds(pl.multiple_of(me * cap, 16), cap)

    def send(step, carry):
        peer = lax.rem(me + step, ring)
        pltpu.make_async_remote_copy(
            src_ref=source.at[pl.ds(pl.multiple_of(peer * cap, 16), cap)],
            dst_ref=target.at[mine],
            send_sem=send_sem,
            recv_sem=recv_sem,
            device_id={"exp": peer},
        ).start()
        return carry

    lax.fori_loop(1, ring, send, 0)
    pltpu.make_async_copy(source.at[mine], target.at[mine], recv_sem).start()


def await_bytes(ref, sem):
    pltpu.make_async_copy(ref, ref, sem).wait()


def spread_kernel(
    windows, ring, ranks, cap,
    upstream, tokens, extended, absent, marks, order, back_order, w_qkv, w_proj,
    out, placers, mixed,
    held, slots, known, queries, keys_values, context,
    z_send, z_recv, m_send, m_recv, a_send, a_recv,
):
    row = lax.axis_index("rep")
    feature = tokens.shape[1]
    enter(ring, ranks)

    def pass_marks(origin, source, side):
        pltpu.make_async_remote_copy(
            src_ref=source,
            dst_ref=known.at[origin],
            send_sem=m_send.at[origin, (side + 1) // 2],
            recv_sem=m_recv.at[origin],
            device_id={"rep": row + side},
        ).start()

    def pass_on(t, origin, source, side):
        pltpu.make_async_remote_copy(
            src_ref=source,
            dst_ref=held.at[t, origin],
            send_sem=z_send.at[t, origin, (side + 1) // 2],
            recv_sem=z_recv.at[t, origin],
            device_id={"rep": row + side},
        ).start()

    def make_placer(origin, ids):
        slot_ids = lax.broadcasted_iota(jnp.int32, placers.shape[1:], 0)
        placers[origin] = (slot_ids == ids).astype(jnp.float32).astype(jnp.bfloat16)

    def dispatch(t, origin, values):
        slots[t, origin] = jnp.dot(
            placers[origin], values, preferred_element_type=jnp.float32
        ).astype(jnp.bfloat16)
        swap_start(
            ring, cap, slots.at[t, origin], out.at[t, origin], a_send.at[t, origin], a_recv.at[t, origin]
        )

    def own(t, source):
        @pl.when(row < ranks - 1)
        def _():
            if t == 0:
                pass_marks(row, marks, 1)
            pass_on(t, row, source, 1)

        @pl.when(row > 0)
        def _():
            if t == 0:
                pass_marks(row, marks, -1)
            pass_on(t, row, source, -1)

        if t == 0:
            make_placer(row, marks[0:1, :])
        dispatch(t, row, source[...])

    def steps(t, begin, end):
        def step(k, carry):
            for side in (1, -1):
                origin = row - side * k

                @pl.when((origin >= 0) & (origin < ranks))
                def _():
                    onward = row + side
                    inner = (onward >= 0) & (onward < ranks)
                    if t == 0:
                        await_bytes(known.at[origin], m_recv.at[origin])

                        @pl.when(inner)
                        def _():
                            pass_marks(origin, known.at[origin], side)

                    await_bytes(held.at[t, origin], z_recv.at[t, origin])

                    @pl.when(inner)
                    def _():
                        pass_on(t, origin, held.at[t, origin], side)

                    if t == 0:
                        make_placer(origin, known[origin, 0:1, :])
                    dispatch(t, origin, held[t, origin])

            return carry

        lax.fori_loop(begin, end, step, 0)

    own(0, upstream)
    keys_values[...] = jnp.dot(
        extended[...], w_qkv[:, feature:], preferred_element_type=jnp.float32
    ).astype(jnp.bfloat16)
    grouped = jnp.dot(order[...], tokens[...], preferred_element_type=jnp.float32)
    queries[...] = jnp.dot(
        grouped.astype(jnp.bfloat16), w_qkv[:, :feature], preferred_element_type=jnp.float32
    ).astype(jnp.bfloat16)
    rounds = 3
    for part in range(rounds):
        low, high = (len(windows) * p // rounds for p in (part, part + 1))
        for number in range(low, high):
            attend_window(number, *windows[number], queries, keys_values, absent, context)
        begin, end = (1 + (ranks - 1) * p // rounds for p in (part, part + 1))
        if part < rounds - 1 and begin < end:
            steps(0, begin, end)
    ungrouped = jnp.dot(back_order[...], context[...], preferred_element_type=jnp.float32)
    attended = jnp.dot(
        ungrouped.astype(jnp.bfloat16), w_proj[...], preferred_element_type=jnp.float32
    )
    mixed[...] = (tokens[...].astype(jnp.float32) + layer_norm(attended)).astype(jnp.bfloat16)
    own(1, mixed)
    steps(0, 1 + (ranks - 1) * (rounds - 1) // rounds, ranks)
    steps(1, 1, ranks)

    def finish(origin, carry):
        for t in range(2):
            await_bytes(out.at[t, origin], a_recv.at[t, origin])
            sent = slots.at[t, origin, pl.ds(0, (ring - 1) * cap)]
            await_bytes(sent, a_send.at[t, origin])

            @pl.when((origin <= row) & (row < ranks - 1))
            def _():
                await_bytes(held.at[t, origin], z_send.at[t, origin, 1])
                if t == 0:
                    await_bytes(known.at[origin], m_send.at[origin, 1])

            @pl.when((origin >= row) & (row > 0))
            def _():
                await_bytes(held.at[t, origin], z_send.at[t, origin, 0])
                if t == 0:
                    await_bytes(known.at[origin], m_send.at[origin, 0])

        return carry

    lax.fori_loop(0, ranks, finish, 0)


def collect_kernel(
    count, ring, ranks, cap, parts, placers, out, back, sums, z_send, z_recv, a_send, a_recv
):
    row = lax.axis_index("rep")
    enter(ring, ranks)

    def launch(t, target):
        swap_start(
            ring, cap, parts[t].at[target], back.at[t, target], a_send.at[t, target], a_recv.at[t, target]
        )

    def ahead(step, carry):
        k = ranks - step
        for t in range(count):
            for side in (1, -1):
                target = row + side * k

                @pl.when((target >= 0) & (target < ranks))
                def _():
                    launch(t, target)

        return carry

    lax.fori_loop(1, ranks, ahead, 0)
    for t in range(count):
        launch(t, row)

    def placed(t, target):
        await_bytes(back.at[t, target], a_recv.at[t, target])
        return lax.dot_general(
            placers[target],
            back[t, target],
            (((0,), (0,)), ((), ())),
            preferred_element_type=jnp.float32,
        )

    def step(index, carry):
        k = ranks - index
        for t in range(count):
            for side in (1, -1):
                target = row + side * k

                @pl.when((target >= 0) & (target < ranks))
                def _():
                    own = placed(t, target)
                    behind = row - side
                    first = (behind < 0) | (behind >= ranks)

                    @pl.when(first)
                    def _():
                        sums[t, target] = own.astype(jnp.bfloat16)

                    @pl.when(jnp.logical_not(first))
                    def _():
                        await_bytes(sums.at[t, target], z_recv.at[t, target])
                        total = own + sums[t, target].astype(jnp.float32)
                        sums[t, target] = total.astype(jnp.bfloat16)

                    final = ranks if side < 0 else target
                    place = jnp.where(k == 1, final, target)
                    pltpu.make_async_remote_copy(
                        src_ref=sums.at[t, target],
                        dst_ref=sums.at[t, place],
                        send_sem=z_send.at[t, target],
                        recv_sem=z_recv.at[t, place],
                        device_id={"rep": row + side},
                    ).start()

        return carry

    lax.fori_loop(1, ranks, step, 0)
    for t in range(count):
        out[t] = placed(t, row)

        @pl.when(row > 0)
        def _():
            await_bytes(sums.at[t, row], z_recv.at[t, row])
            out[t] += sums[t, row].astype(jnp.float32)

        @pl.when(row < ranks - 1)
        def _():
            await_bytes(sums.at[t, ranks], z_recv.at[t, ranks])
            out[t] += sums[t, ranks].astype(jnp.float32)

    def finish(target, carry):
        for t in range(count):
            sent = back.at[t, target, pl.ds(0, (ring - 1) * cap)]
            await_bytes(sent, a_send.at[t, target])

            @pl.when(target != row)
            def _():
                await_bytes(sums.at[t, target], z_send.at[t, target])

        return carry

    lax.fori_loop(0, ranks, finish, 0)


def in_vmem(amount):
    return [pl.BlockSpec(memory_space=pltpu.VMEM)] * amount


def spread(operands, windows, ring, ranks, cap):
    tok, feature = operands[1].shape
    ext_count = operands[2].shape[0]
    rows = ring * cap

    def body(*refs):
        spread_kernel(windows, ring, ranks, cap, *refs)

    return pl.pallas_call(
        body,
        name="spread",
        out_shape=(
            jax.ShapeDtypeStruct((2, ranks, rows, feature), jnp.bfloat16),
            jax.ShapeDtypeStruct((ranks, rows, tok), jnp.bfloat16),
            jax.ShapeDtypeStruct((tok, feature), jnp.bfloat16),
        ),
        in_specs=in_vmem(len(operands)),
        out_specs=tuple(in_vmem(3)),
        scratch_shapes=[
            pltpu.VMEM((2, ranks, tok, feature), jnp.bfloat16),
            pltpu.VMEM((2, ranks, rows, feature), jnp.bfloat16),
            pltpu.VMEM((ranks, 8, tok), jnp.int32),
            pltpu.VMEM((tok, feature), jnp.bfloat16),
            pltpu.VMEM((ext_count, 2 * feature), jnp.bfloat16),
            pltpu.VMEM((tok, feature), jnp.bfloat16),
            pltpu.SemaphoreType.DMA((2, ranks, 2)),
            pltpu.SemaphoreType.DMA((2, ranks)),
            pltpu.SemaphoreType.DMA((ranks, 2)),
            pltpu.SemaphoreType.DMA((ranks,)),
            pltpu.SemaphoreType.DMA((2, ranks)),
            pltpu.SemaphoreType.DMA((2, ranks)),
        ],
        compiler_params=pltpu.CompilerParams(
            collective_id=0, has_side_effects=True, vmem_limit_bytes=60 << 20
        ),
    )(*operands)


def collect(parts, placers, ring, ranks, cap):
    count = len(parts)
    rows, feature = parts[0].shape[1:]
    tok = placers.shape[2]

    def body(*refs):
        collect_kernel(count, ring, ranks, cap, refs[:count], *refs[count:])

    return pl.pallas_call(
        body,
        name="collect",
        out_shape=jax.ShapeDtypeStruct((count, tok, feature), jnp.float32),
        in_specs=in_vmem(count + 1),
        out_specs=pl.BlockSpec(memory_space=pltpu.VMEM),
        scratch_shapes=[
            pltpu.VMEM((count, ranks, rows, feature), jnp.bfloat16),
            pltpu.VMEM((count, ranks + 1, tok, feature), jnp.bfloat16),
            pltpu.SemaphoreType.DMA((count, ranks)),
            pltpu.SemaphoreType.DMA((count, ranks + 1)),
            pltpu.SemaphoreType.DMA((count, ranks)),
            pltpu.SemaphoreType.DMA((count, ranks)),
        ],
        compiler_params=pltpu.CompilerParams(
            collective_id=1, has_side_effects=True, vmem_limit_bytes=60 << 20
        ),
    )(*parts, placers)


def per_device(tokens, gate, route, cotangent, w_qkv, w_proj, w_up, w_down):
    tile_rows, tile_cols, feature = tokens.shape
    tok_count = tile_rows * tile_cols
    ext_rows = tile_rows + 2 * margin_cells
    ext_cols = tile_cols + 2 * margin_cells
    extended = padded(tokens, (("rep", 0), ("exp", 1)), 4)
    win_rows, win_cols = ext_rows // window_side, ext_cols // window_side

    def by_window(cells):
        split = cells.reshape(win_rows, window_side, win_cols, window_side, -1)
        return split.transpose(0, 2, 1, 3, 4).reshape(win_rows * win_cols, window_side**2, -1)

    row_ids = (
        lax.axis_index("rep") * tile_rows - margin_cells + jnp.arange(ext_rows, dtype=jnp.int32)
    )
    col_ids = (
        lax.axis_index("exp") * tile_cols - margin_cells + jnp.arange(ext_cols, dtype=jnp.int32)
    )
    row_inside = (row_ids >= 0) & (row_ids < tile_rows * lax.axis_size("rep"))
    col_inside = (col_ids >= 0) & (col_ids < tile_cols * lax.axis_size("exp"))
    in_grid = row_inside[:, None] & col_inside[None, :]
    absent = jnp.where(by_window(in_grid)[..., 0], 0.0, -1e30).astype(jnp.float32)
    flat_tokens = tokens.reshape(tok_count, feature)
    order, windows = window_order(tile_rows, tile_cols)
    grouping = np.zeros((tok_count, tok_count), np.float32)
    grouping[np.arange(tok_count), order] = 1.0
    grouping = jnp.asarray(grouping, jnp.bfloat16)
    experts = lax.axis_size("exp")
    ranks = lax.axis_size("rep")
    capacity = max(2, 3 * tok_count // (2 * experts))
    capacity = -(-capacity // 16) * 16
    slot_count = experts * capacity
    chosen = route.reshape(tok_count)
    matches = (chosen[:, None] == jnp.arange(experts, dtype=jnp.int32)[None, :]).astype(jnp.int32)
    position = jnp.sum(matches * (jnp.cumsum(matches, axis=0) - 1), axis=1)
    marks = jnp.broadcast_to((chosen * capacity + position)[None, :], (8, tok_count))
    gate_rows = gate.reshape(tok_count)
    upstream = (
        gate_rows[:, None] * cotangent.reshape(tok_count, feature).astype(jnp.float32)
    ).astype(jnp.bfloat16)
    operands = (
        upstream,
        flat_tokens,
        by_window(extended).reshape(-1, feature),
        absent,
        marks,
        grouping,
        grouping.T,
        w_qkv,
        w_proj,
    )
    gathered, placers, mixed = spread(operands, windows, experts, ranks, capacity)
    slot_grads = gathered[0].reshape(-1, feature)
    slot_rows = gathered[1].reshape(-1, feature)
    up_mat = w_up[0]
    down_mat = w_down[0]
    pre_act = lax.dot_general(
        slot_rows, up_mat, (((1,), (1,)), ((), ())), preferred_element_type=jnp.float32
    )
    hidden = gelu_tanh(pre_act).astype(jnp.bfloat16)
    expert_out = jnp.dot(hidden, down_mat, preferred_element_type=jnp.float32).astype(jnp.bfloat16)
    hidden_grad = lax.dot_general(
        slot_grads, down_mat, (((1,), (1,)), ((), ())), preferred_element_type=jnp.float32
    )
    pre_grad = (hidden_grad * gelu_slope(pre_act)).astype(jnp.bfloat16)
    input_slots = jnp.dot(pre_grad, up_mat, preferred_element_type=jnp.float32).astype(jnp.bfloat16)
    shape = (ranks, slot_count, feature)
    returned = collect(
        (expert_out.reshape(shape), input_slots.reshape(shape)), placers, experts, ranks, capacity
    )
    layer_out = (mixed.astype(jnp.float32) + gate_rows[:, None] * returned[0]).astype(jnp.bfloat16)
    input_grad = returned[1].astype(jnp.bfloat16)
    average_factor = 1.0 / ranks
    grad_up = lax.dot_general(
        pre_grad, slot_rows, (((0,), (0,)), ((), ())), preferred_element_type=jnp.float32
    )
    grad_down = lax.dot_general(
        hidden, slot_grads, (((0,), (0,)), ((), ())), preferred_element_type=jnp.float32
    )
    return (
        layer_out.reshape(tile_rows, tile_cols, feature),
        input_grad.reshape(tile_rows, tile_cols, feature),
        (grad_up * average_factor)[None],
        (grad_down * average_factor)[None],
    )


def solution(mesh):
    placed = (
        P("rep", "exp", None),
        P("rep", "exp"),
        P("rep", "exp", None, None),
        P("rep", "exp", None),
        P(),
        P(),
        P("exp", "rep", None),
        P("exp", "rep", None),
    )
    return jax.shard_map(
        per_device,
        mesh=mesh,
        in_specs=placed,
        out_specs=(
            P("rep", "exp", None),
            P("rep", "exp", None),
            P("exp", "rep", None),
            P("exp", "rep", None),
        ),
        check_vma=False,
    )
```
